32 devices in a mesh: dp: 2 (over x), ep: 16 (over z, y, core).
Axes of the slice: x: 2, y: 2, z: 4, core: 2. Of those that a mesh axis runs over, the one named last changes fastest.
Arguments:
- dy_home: bfloat16 [4096, 1024], P(('dp', 'ep')), parts along dimension 0
- topk_idx: int32 [4096, 8], P(('dp', 'ep')), parts along dimension 0
- slot_idx: int32 [4096, 8], P(('dp', 'ep')), parts along dimension 0
- gates: float32 [4096, 8], P(('dp', 'ep')), parts along dimension 0
- y_back: bfloat16 [4096, 8, 1024], P(('dp', 'ep')), parts along dimension 0
- x_disp: bfloat16 [64, 1024, 1024], P(('dp', 'ep')), parts along dimension 0
- h1_disp: bfloat16 [64, 1024, 512], P(('dp', 'ep')), parts along dimension 0
- h3_disp: bfloat16 [64, 1024, 512], P(('dp', 'ep')), parts along dimension 0
- w_gate: bfloat16 [32, 1024, 512], P('ep')
- w_up: bfloat16 [32, 1024, 512], P('ep')
- w_down: bfloat16 [32, 512, 1024], P('ep')
Outputs:
- output 1: bfloat16 [4096, 1024], P(('dp', 'ep')), parts along dimension 0
- output 2: float32 [4096, 8], P(('dp', 'ep')), parts along dimension 0
- output 3: float32 [64, 1024, 512], P(('dp', 'ep')), parts along dimension 0
- output 4: float32 [64, 1024, 512], P(('dp', 'ep')), parts along dimension 0
- output 5: float32 [64, 512, 1024], P(('dp', 'ep')), parts along dimension 0
There are 2 independent parts. The reference program is written for one: setup_inputs(seed, part) draws one part's arguments, and reference() takes and returns one part's arrays. A program takes and returns all parts, laid end to end along the dimension named above; an argument that names none is the same for every part.
All inputs are finite; a program needn't handle non-finite values.
Results may differ from the reference program's by a relative error of at most 0.0149638.
Values are sent between devices in bfloat16 or wider.
A program may use at most 1 GiB of HBM per device.

```python
import jax
import jax.numpy as jnp
from jax import lax

EP_SIZE = 16
TOKENS_DEV = 128
TOP = 8
EXPERTS = 32
D = 1024
FF = 512

CAPACITY = 2 * TOKENS_DEV * TOP // EXPERTS
ALL_TOKENS = EP_SIZE * TOKENS_DEV
ROWS_ALL = EXPERTS * EP_SIZE * CAPACITY


def rank_in_buffer(expert_ids):
    num_items = TOKENS_DEV * TOP
    positions = jnp.arange(num_items, dtype=jnp.int32)
    sort_order = jnp.argsort(expert_ids * num_items + positions)
    sorted_ids = expert_ids[sort_order]
    first_pos = jnp.searchsorted(sorted_ids, sorted_ids, side='left').astype(jnp.int32)
    buf_rank = jnp.zeros((num_items,), jnp.int32).at[sort_order].set(positions - first_pos)
    return jnp.where(buf_rank < CAPACITY, buf_rank, -1)


def route_draw(route_key):
    key_base, key_bias, key_hot = jax.random.split(route_key, 3)
    base_score = jax.random.randint(key_base, (ALL_TOKENS, EXPERTS), 0, 65536)
    expert_bias = jax.random.randint(key_bias, (EXPERTS,), 0, 32768)
    hot_expert = jax.random.randint(key_hot, (), 0, EXPERTS)
    tok_pos = jnp.arange(ALL_TOKENS, dtype=jnp.int32) % TOKENS_DEV
    expert_ids = jnp.arange(EXPERTS, dtype=jnp.int32)
    forced = (tok_pos[:, None] <= CAPACITY) & (expert_ids[None, :] == hot_expert)
    full_score = (base_score + expert_bias[None, :] + jnp.where(forced, 131072, 0)) * EXPERTS + expert_ids[None, :]
    topk_idx = lax.top_k(full_score, TOP)[1].astype(jnp.int32)
    slot_idx = jax.vmap(rank_in_buffer)(topk_idx.reshape(EP_SIZE, TOKENS_DEV * TOP))
    return topk_idx, slot_idx.reshape(ALL_TOKENS, TOP)


def buffer_index(topk_idx, slot_idx):
    src_dev = jnp.arange(ALL_TOKENS, dtype=jnp.int32) // TOKENS_DEV
    flat_pos = (topk_idx * EP_SIZE + src_dev[:, None]) * CAPACITY + slot_idx
    return jnp.where(slot_idx >= 0, flat_pos, ROWS_ALL)


def expert_forward(operands):
    x_expert, gate_w, up_w, down_w = operands
    h_gate = jnp.dot(x_expert, gate_w, preferred_element_type=jnp.float32).astype(jnp.bfloat16)
    h_up = jnp.dot(x_expert, up_w, preferred_element_type=jnp.float32).astype(jnp.bfloat16)
    hidden_act = (jax.nn.silu(h_gate.astype(jnp.float32)) * h_up.astype(jnp.float32)).astype(jnp.bfloat16)
    y_expert = jnp.dot(hidden_act, down_w, preferred_element_type=jnp.float32).astype(jnp.bfloat16)
    return h_gate, h_up, y_expert


def forward_buffers(x_tok, flat_pos, w_gate, w_up, w_down):
    x_rows = jnp.broadcast_to(x_tok[:, None, :], (ALL_TOKENS, TOP, D)).reshape(ALL_TOKENS * TOP, D)
    x_disp = jnp.zeros((ROWS_ALL, D), jnp.bfloat16).at[flat_pos.reshape(-1)].set(x_rows, mode='drop')
    x_disp = x_disp.reshape(EXPERTS, EP_SIZE * CAPACITY, D)
    h1_disp, h3_disp, y_disp = lax.map(expert_forward, (x_disp, w_gate, w_up, w_down))
    y_back = jnp.take(y_disp.reshape(ROWS_ALL, D), flat_pos, axis=0, mode='fill', fill_value=0)
    return y_back, x_disp, h1_disp, h3_disp


def setup_inputs(seed: int = 0, part: int = 0) -> dict:
    root_key = jax.random.key(seed)
    key_gate, key_up, key_down = jax.random.split(root_key, 3)
    w_gate = (jax.random.normal(key_gate, (EXPERTS, D, FF), jnp.float32) * D ** -0.5).astype(jnp.bfloat16)
    w_up = (jax.random.normal(key_up, (EXPERTS, D, FF), jnp.float32) * D ** -0.5).astype(jnp.bfloat16)
    w_down = (jax.random.normal(key_down, (EXPERTS, FF, D), jnp.float32) * FF ** -0.5).astype(jnp.bfloat16)
    part_key = jax.random.fold_in(root_key, part)
    key_route, key_tok, key_grad, key_mix = jax.random.split(part_key, 4)
    topk_idx, slot_idx = route_draw(key_route)
    gates = jax.random.uniform(key_mix, (ALL_TOKENS, TOP), jnp.float32, 0.2, 1.0)
    x_tok = jax.random.normal(key_tok, (ALL_TOKENS, D), jnp.float32).astype(jnp.bfloat16)
    dy_home = jax.random.normal(key_grad, (ALL_TOKENS, D), jnp.float32).astype(jnp.bfloat16)
    flat_pos = buffer_index(topk_idx, slot_idx)
    y_back, x_disp, h1_disp, h3_disp = forward_buffers(x_tok, flat_pos, w_gate, w_up, w_down)
    return {'dy_home': dy_home, 'topk_idx': topk_idx, 'slot_idx': slot_idx, 'gates': gates,
            'y_back': y_back, 'x_disp': x_disp, 'h1_disp': h1_disp, 'h3_disp': h3_disp,
            'w_gate': w_gate, 'w_up': w_up, 'w_down': w_down}


def expert_backward(operands):
    dy_expert, x_expert, h_gate, h_up, gate_w, up_w, down_w = operands
    gate_f = h_gate.astype(jnp.float32)
    up_f = h_up.astype(jnp.float32)
    sig_gate = jax.nn.sigmoid(gate_f)
    silu_g = gate_f * sig_gate
    hidden_act = (silu_g * up_f).astype(jnp.bfloat16)
    d_act = jnp.dot(dy_expert, down_w.T, preferred_element_type=jnp.float32).astype(jnp.bfloat16).astype(jnp.float32)
    dh_gate = (d_act * up_f * sig_gate * (1.0 + gate_f * (1.0 - sig_gate))).astype(jnp.bfloat16)
    dh_up = (d_act * silu_g).astype(jnp.bfloat16)
    dw_down = jnp.dot(hidden_act.T, dy_expert, preferred_element_type=jnp.float32)
    dw_gate = jnp.dot(x_expert.T, dh_gate, preferred_element_type=jnp.float32)
    dw_up = jnp.dot(x_expert.T, dh_up, preferred_element_type=jnp.float32)
    dx_expert = (jnp.dot(dh_gate, gate_w.T, preferred_element_type=jnp.float32)
                 + jnp.dot(dh_up, up_w.T, preferred_element_type=jnp.float32)).astype(jnp.bfloat16)
    return dx_expert, dw_gate, dw_up, dw_down


def reference(dy_home, topk_idx, slot_idx, gates, y_back, x_disp, h1_disp, h3_disp, w_gate, w_up, w_down):
    d_gates = jnp.einsum('td,tjd->tj', dy_home.astype(jnp.float32), y_back.astype(jnp.float32))
    flat_pos = buffer_index(topk_idx, slot_idx)
    gated_rows = (gates[:, :, None] * dy_home[:, None, :].astype(jnp.float32)).astype(jnp.bfloat16)
    dy_disp = jnp.zeros((ROWS_ALL, D), jnp.bfloat16).at[flat_pos.reshape(-1)].set(gated_rows.reshape(ALL_TOKENS * TOP, D), mode='drop')
    dy_disp = dy_disp.reshape(EXPERTS, EP_SIZE * CAPACITY, D)
    dx_disp, dw_gate, dw_up, dw_down = lax.map(expert_backward, (dy_disp, x_disp, h1_disp, h3_disp, w_gate, w_up, w_down))
    returned = jnp.take(dx_disp.reshape(ROWS_ALL, D), flat_pos, axis=0, mode='fill', fill_value=0)
    dx_home = jnp.sum(returned.astype(jnp.float32), axis=1).astype(jnp.bfloat16)
    return dx_home, d_gates, dw_gate, dw_up, dw_down
```

```python
import functools

import jax
import jax.numpy as jnp
from jax import lax
from jax.experimental import pallas as pl
from jax.experimental.pallas import tpu as pltpu
from jax.sharding import PartitionSpec as P

MESH = pl.DeviceIdType.MESH
F32 = jnp.float32
BF16 = jnp.bfloat16
NZ = 4
NR = 2


def line_pos(z, k):
    edge = z * (3 - z) // 2
    far = z // 2
    is0 = (3 - k) // 3
    is1 = (k + 2) // 3 - (k + 1) // 3
    q = k + edge * is0 - edge * is1
    return q + 3 * far - 2 * far * q


def dot_t(a, b):
    return lax.dot_general(a, b, (((1,), (1,)), ((), ())), preferred_element_type=F32)


def exchange_kernel(tok, cap, top,
                    dy_ref, meta_ref, h1_hbm, h3_hbm, wg_hbm, wu_hbm, wd_hbm,
                    dx_ref, dyd_hbm, act_hbm, dh1_hbm, dh3_hbm,
                    gat, met, h1, h3, wg, wu, wd, dyd, act, dh1, dh3, xd, xr,
                    own, sy, ry, sz, rz,
                    load_sem, out_sem, ag_send, ag_recv, mt_send, mt_recv,
                    xs_sem, xr_sem, sy_sem, ry_sem, sz_sem, rz_sem):
    me = lax.axis_index('ep')
    dp = lax.axis_index('dp')
    z, y, c = me // 4, (me // 2) % 2, me % 2
    oy, oc = 1 - y, 1 - c

    def dev(z_, y_, c_):
        return (dp, (z_ * 2 + y_) * 2 + c_)

    def home(z_, y_, c_):
        return (z_ * 2 + y_) * 2 + c_

    loads = [pltpu.make_async_copy(s, d, load_sem.at[i]) for i, (s, d) in enumerate(
        ((wd_hbm, wd), (h1_hbm, h1), (h3_hbm, h3), (wg_hbm, wg), (wu_hbm, wu)))]
    for cp in loads:
        cp.start()

    barrier = pltpu.get_barrier_semaphore()
    pl.semaphore_signal(barrier, inc=1, device_id=dev(z, y, oc), device_id_type=MESH)
    pl.semaphore_signal(barrier, inc=1, device_id=dev(z, oy, c), device_id_type=MESH)

    @pl.when(z > 0)
    def _():
        pl.semaphore_signal(barrier, inc=1, device_id=dev(z - 1, y, c), device_id_type=MESH)

    @pl.when(z < NZ - 1)
    def _():
        pl.semaphore_signal(barrier, inc=1, device_id=dev(z + 1, y, c), device_id_type=MESH)

    pl.semaphore_wait(barrier, 3 + z * (NZ - 1 - z) // 2)

    def ag_copies(src, msrc, hid, way, target):
        return (pltpu.make_async_remote_copy(src, gat.at[hid], ag_send.at[hid, way], ag_recv.at[hid],
                                             device_id=target, device_id_type=MESH),
                pltpu.make_async_remote_copy(msrc, met.at[hid], mt_send.at[hid, way], mt_recv.at[hid],
                                             device_id=target, device_id_type=MESH))

    def start(copies):
        for cp in copies:
            cp.start()

    def ag_wait(hid):
        for cp in ag_copies(gat.at[hid], met.at[hid], hid, 0, dev(z, y, oc)):
            cp.wait_recv()

    @pl.when(z < NZ - 1)
    def _():
        start(ag_copies(dy_ref, meta_ref, me, 2, dev(z + 1, y, c)))

    @pl.when(z > 0)
    def _():
        start(ag_copies(dy_ref, meta_ref, me, 3, dev(z - 1, y, c)))

    start(ag_copies(dy_ref, meta_ref, me, 1, dev(z, oy, c)))
    start(ag_copies(dy_ref, meta_ref, me, 0, dev(z, y, oc)))
    gat[me] = dy_ref[...]
    met[me] = meta_ref[...]

    def from_line(k):
        p = line_pos(z, k)
        hid = home(p, y, c)
        ag_wait(hid)
        blk, mblk = gat.at[hid], met.at[hid]

        @pl.when((p < z) & (z < NZ - 1))
        def _():
            start(ag_copies(blk, mblk, hid, 2, dev(z + 1, y, c)))

        @pl.when((p > z) & (z > 0))
        def _():
            start(ag_copies(blk, mblk, hid, 3, dev(z - 1, y, c)))

        start(ag_copies(blk, mblk, hid, 1, dev(z, oy, c)))
        start(ag_copies(blk, mblk, hid, 0, dev(z, y, oc)))

    def from_pair(k):
        hid = home(line_pos(z, k), oy, c)
        ag_wait(hid)
        start(ag_copies(gat.at[hid], met.at[hid], hid, 0, dev(z, y, oc)))

    for cp in loads:
        cp.wait()

    def xs_copy(chip):
        return pltpu.make_async_remote_copy(xd.at[chip, oc], xr.at[chip], xs_sem.at[chip], xr_sem.at[chip],
                                            device_id=dev(z, y, oc), device_id_type=MESH)

    def out_copies(chip):
        rows = pl.ds(chip * 2 * cap, 2 * cap)
        return [pltpu.make_async_copy(s.at[:, rows], d.at[:, rows], out_sem.at[i, chip]) for i, (s, d) in enumerate(
            ((dyd, dyd_hbm), (act, act_hbm), (dh1, dh1_hbm), (dh3, dh3_hbm)))]

    slot = lax.broadcasted_iota(jnp.int32, (cap, 1), 0).astype(F32)

    def group(chip):
        first = (me * 2 * cap).astype(F32)
        rows = pl.ds(chip * 2 * cap, 2 * cap)
        picks, row_gate = [], []
        for e in range(2):
            for h in range(2):
                want = slot + (first + float(e * cap))
                hit = jnp.zeros((cap, tok), F32)
                gsum = jnp.zeros((cap, tok), F32)
                for j in range(top):
                    same = met[chip * 2 + h, j:j + 1, :] == want
                    hit = jnp.where(same, 1.0, hit)
                    gsum = jnp.where(same, met[chip * 2 + h, top + j:top + j + 1, :], gsum)
                row_gate.append(jnp.sum(gsum, axis=1, keepdims=True))
                none = jnp.zeros((cap, tok), F32)
                picks.append(jnp.concatenate([hit, none] if h == 0 else [none, hit], axis=1))
        pick = jnp.concatenate(picks, axis=0).astype(BF16)
        gate = jnp.concatenate(row_gate, axis=0)
        pair = jnp.concatenate([gat[chip * 2], gat[chip * 2 + 1]], axis=0)
        picked = jnp.dot(pick, pair, preferred_element_type=F32)
        rows_dy = (picked * gate).astype(BF16)
        for e in range(2):
            dy_e = rows_dy[e * 2 * cap:(e + 1) * 2 * cap]
            dyd[e, rows] = dy_e
            d_act = dot_t(dy_e, wd[e]).astype(BF16).astype(F32)
            gate_f = h1[e, rows].astype(F32)
            up_f = h3[e, rows].astype(F32)
            sig = jax.nn.sigmoid(gate_f)
            silu = gate_f * sig
            act[e, rows] = (silu * up_f).astype(BF16)
            d1 = (d_act * up_f * sig * (1.0 + gate_f * (1.0 - sig))).astype(BF16)
            d3 = (d_act * silu).astype(BF16)
            dh1[e, rows] = d1
            dh3[e, rows] = d3
            d_x = (dot_t(d1, wg[e]) + dot_t(d3, wu[e])).astype(BF16)
            for h in range(2):
                xd[chip, h, e * cap:(e + 1) * cap] = d_x[h * cap:(h + 1) * cap]
        xs_copy(chip).start()
        for cp in out_copies(chip):
            cp.start()

    def step(n, carry):
        k, side = n // 2, n % 2

        @pl.when((side == 0) & (k < NZ - 1))
        def _():
            from_line(k + 1)
            from_pair(k)

        @pl.when((side == 1) & (k == NZ - 1))
        def _():
            from_pair(k)

        yy = y + side - 2 * y * side
        p = line_pos(z, k)
        ag_wait(home(p, yy, oc))
        group(p * 2 + yy)
        return carry

    lax.fori_loop(0, 2 * NZ, step, 0)

    row_id = lax.broadcasted_iota(jnp.int32, (2 * cap, 1), 0).astype(F32)

    def partial(chip):
        hid = chip * 2 + c
        xs_copy(chip).wait_recv()
        want = jnp.concatenate([row_id + (me * 2 * cap).astype(F32),
                                row_id + ((me + 1 - 2 * c) * 2 * cap).astype(F32)], axis=0)
        hit = jnp.zeros((4 * cap, tok), F32)
        for j in range(top):
            hit = jnp.where(met[hid, j:j + 1, :] == want, 1.0, hit)
        vals = jnp.concatenate([xd[chip, c], xr[chip]], axis=0)
        return lax.dot_general(hit.astype(BF16), vals, (((0,), (0,)), ((), ())), preferred_element_type=F32)

    half = tok // NR

    def y_copy(k, i):
        return pltpu.make_async_remote_copy(sy.at[k, i], ry.at[k, i], sy_sem.at[k, i], ry_sem.at[k, i],
                                            device_id=dev(z, oy, c), device_id_type=MESH)

    def z_copy(k, i, target_z, to_slot):
        return pltpu.make_async_remote_copy(sz.at[k, i], rz.at[to_slot, i], sz_sem.at[k, i], rz_sem.at[to_slot, i],
                                            device_id=dev(target_z, y, c), device_id_type=MESH)

    def z_wait(from_slot, i):
        z_copy(0, i, z, from_slot).wait_recv()

    for k in (3, 2, 1, 0):
        part = partial(line_pos(z, k) * 2 + oy)
        for i in range(NR):
            sy[k, i] = part[i * half:(i + 1) * half]
            y_copy(k, i).start()

    for k in (3, 1, 2):
        p = line_pos(z, k)
        way = jnp.where(p > z, 1, -1)
        own[...] = partial(p * 2 + y)
        behind = z - way
        has_in = (behind >= 0) & (behind < NZ)
        ahead = z + way
        to_slot = jnp.where(ahead == p, jnp.where(way > 0, NZ, NZ + 1), p)
        for i in range(NR):
            y_copy(k, i).wait_recv()
            sz[k, i] = own[i * half:(i + 1) * half] + ry[k, i]

            @pl.when(has_in)
            def _():
                z_wait(p, i)
                sz[k, i] += rz[p, i]

            z_copy(k, i, ahead, to_slot).start()

    own[...] = partial(z * 2 + y)
    for i in range(NR):
        rows = slice(i * half, (i + 1) * half)
        y_copy(0, i).wait_recv()
        own[rows] += ry[0, i]

        @pl.when(z > 0)
        def _():
            z_wait(NZ, i)
            own[rows] += rz[NZ, i]

        @pl.when(z < NZ - 1)
        def _():
            z_wait(NZ + 1, i)
            own[rows] += rz[NZ + 1, i]

        dx_ref[rows] = own[rows].astype(BF16)

    def ag_sent(hid, way):
        for cp in ag_copies(gat.at[hid], met.at[hid], hid, way, dev(z, y, oc)):
            cp.wait_send()

    for k in range(NZ):
        p = line_pos(z, k)
        hid = home(p, y, c)
        ag_sent(hid, 0)
        ag_sent(hid, 1)
        ag_sent(home(p, oy, c), 0)

        @pl.when((p <= z) & (z < NZ - 1))
        def _():
            ag_sent(hid, 2)

        @pl.when((p >= z) & (z > 0))
        def _():
            ag_sent(hid, 3)

        for i in range(NR):
            y_copy(k, i).wait_send()
            if k:
                z_copy(k, i, z, 0).wait_send()

    def drain(chip, carry):
        xs_copy(chip).wait_send()
        for cp in out_copies(chip):
            cp.wait()
        return carry

    lax.fori_loop(0, 2 * NZ, drain, 0)


def exchange(dy, meta, h1, h3, wg, wu, wd, cap, top):
    tok, width = dy.shape
    n_exp, rows, ff = h1.shape
    homes = rows // cap
    chips = homes // 2
    half = tok // NR
    dma = pltpu.SemaphoreType.DMA
    any_spec = pl.BlockSpec(memory_space=pl.ANY)
    vmem_spec = pl.BlockSpec(memory_space=pltpu.VMEM)
    return pl.pallas_call(
        functools.partial(exchange_kernel, tok, cap, top),
        out_shape=(jax.ShapeDtypeStruct((tok, width), BF16),
                   jax.ShapeDtypeStruct((n_exp, rows, width), BF16),
                   jax.ShapeDtypeStruct((n_exp, rows, ff), BF16),
                   jax.ShapeDtypeStruct((n_exp, rows, ff), BF16),
                   jax.ShapeDtypeStruct((n_exp, rows, ff), BF16)),
        in_specs=[vmem_spec] * 2 + [any_spec] * 5,
        out_specs=(vmem_spec,) + (any_spec,) * 4,
        scratch_shapes=[
            pltpu.VMEM((homes, tok, width), BF16),
            pltpu.VMEM((homes, 2 * top, tok), F32),
            pltpu.VMEM(h1.shape, BF16),
            pltpu.VMEM(h3.shape, BF16),
            pltpu.VMEM(wg.shape, BF16),
            pltpu.VMEM(wu.shape, BF16),
            pltpu.VMEM(wd.shape, BF16),
            pltpu.VMEM((n_exp, rows, width), BF16),
            pltpu.VMEM((n_exp, rows, ff), BF16),
            pltpu.VMEM((n_exp, rows, ff), BF16),
            pltpu.VMEM((n_exp, rows, ff), BF16),
            pltpu.VMEM((chips, 2, n_exp * cap, width), BF16),
            pltpu.VMEM((chips, n_exp * cap, width), BF16),
            pltpu.VMEM((tok, width), F32),
            pltpu.VMEM((NZ, NR, half, width), F32),
            pltpu.VMEM((NZ, NR, half, width), F32),
            pltpu.VMEM((NZ, NR, half, width), F32),
            pltpu.VMEM((NZ + 2, NR, half, width), F32),
            dma((5,)), dma((4, chips)),
            dma((homes, 4)), dma((homes,)), dma((homes, 4)), dma((homes,)),
            dma((chips,)), dma((chips,)),
            dma((NZ, NR)), dma((NZ, NR)), dma((NZ, NR)), dma((NZ + 2, NR)),
        ],
        compiler_params=pltpu.CompilerParams(
            collective_id=0, has_side_effects=True, vmem_limit_bytes=62 * 2 ** 20),
    )(dy, meta, h1, h3, wg, wu, wd)


def weight_kernel(x_ref, dyd_ref, act_ref, dh1_ref, dh3_ref, gate_ref, up_ref, down_ref):
    def dot_0(a, b):
        return lax.dot_general(a, b, (((0,), (0,)), ((), ())), preferred_element_type=F32)

    gate_ref[0] = dot_0(x_ref[0], dh1_ref[0])
    up_ref[0] = dot_0(x_ref[0], dh3_ref[0])
    down_ref[0] = dot_0(act_ref[0], dyd_ref[0])


def weight_grads(x, dyd, act, dh1, dh3):
    n_exp, rows, width = x.shape
    ff = act.shape[2]
    tile = 256
    wide = pl.BlockSpec((1, rows, tile), lambda e, i: (e, 0, i))
    full = pl.BlockSpec((1, rows, ff), lambda e, i: (e, 0, 0))
    return pl.pallas_call(
        weight_kernel,
        grid=(n_exp, width // tile),
        in_specs=[wide, wide, full, full, full],
        out_specs=(pl.BlockSpec((1, tile, ff), lambda e, i: (e, i, 0)),
                   pl.BlockSpec((1, tile, ff), lambda e, i: (e, i, 0)),
                   pl.BlockSpec((1, ff, tile), lambda e, i: (e, 0, i))),
        out_shape=(jax.ShapeDtypeStruct((n_exp, width, ff), F32),
                   jax.ShapeDtypeStruct((n_exp, width, ff), F32),
                   jax.ShapeDtypeStruct((n_exp, ff, width), F32)),
        compiler_params=pltpu.CompilerParams(
            dimension_semantics=('arbitrary', 'arbitrary'), vmem_limit_bytes=60 * 2 ** 20),
    )(x, dyd, act, dh1, dh3)


def solution(mesh):
    ep_size = mesh.shape['ep']
    tok_spec = P(('dp', 'ep'), None)
    buf_spec = P(('dp', 'ep'), None, None)
    expert_spec = P('ep', None, None)

    def device_step(dy_loc, topk_idx, slot_idx, gates, y_back, x_disp, h1_disp, h3_disp, w_gate, w_up, w_down):
        cap = x_disp.shape[1] // ep_size
        top = topk_idx.shape[1]
        d_gates = jnp.einsum('td,tjd->tj', dy_loc, y_back, preferred_element_type=F32)
        flat = jnp.where(slot_idx >= 0, topk_idx * cap + slot_idx, -1).astype(F32)
        meta = jnp.concatenate([flat.T, gates.T], axis=0)
        dx_loc, dyd, act, dh1, dh3 = exchange(dy_loc, meta, h1_disp, h3_disp, w_gate, w_up, w_down, cap, top)
        dw_gate, dw_up, dw_down = weight_grads(x_disp, dyd, act, dh1, dh3)
        return dx_loc, d_gates, dw_gate, dw_up, dw_down

    return jax.shard_map(
        device_step, mesh=mesh,
        in_specs=(tok_spec, tok_spec, tok_spec, tok_spec, buf_spec, buf_spec, buf_spec, buf_spec,
                  expert_spec, expert_spec, expert_spec),
        out_specs=(tok_spec, tok_spec, buf_spec, buf_spec, buf_spec),
        check_vma=False)
```

```python
import functools

import jax
import jax.numpy as jnp
from jax import lax
from jax.experimental import pallas as pl
from jax.experimental.pallas import tpu as pltpu
from jax.sharding import PartitionSpec as P

MESH = pl.DeviceIdType.MESH
F32 = jnp.float32
BF16 = jnp.bfloat16
NZ = 4
NR = 4


def line_pos(z, k):
    edge = z * (3 - z) // 2
    far = z // 2
    is0 = (3 - k) // 3
    is1 = (k + 2) // 3 - (k + 1) // 3
    q = k + edge * is0 - edge * is1
    return q + 3 * far - 2 * far * q


def dot(a, b):
    return jnp.dot(a, b, preferred_element_type=F32)


def exchange_kernel(tok, cap, top,
                    dy_ref, meta_ref, h1_hbm, h3_hbm, wg_hbm, wu_hbm, wd_hbm,
                    dx_ref, dyd_hbm, act_hbm, dh1_hbm, dh3_hbm,
                    gat, met, h1, h3, wg, wu, wd, wg_t, wu_t, wd_t, dyd, act, dh1, dh3, xd, xr,
                    sp, ry, rz,
                    load_sem, out_sem, ag_send, ag_recv, mt_send, mt_recv,
                    xs_sem, xr_sem, sy_sem, ry_sem, sz_sem, rz_sem):
    me = lax.axis_index('ep')
    dp = lax.axis_index('dp')
    z, y, c = me // 4, (me // 2) % 2, me % 2
    oy, oc = 1 - y, 1 - c

    def dev(z_, y_, c_):
        return (dp, (z_ * 2 + y_) * 2 + c_)

    def home(z_, y_, c_):
        return (z_ * 2 + y_) * 2 + c_

    loads = [pltpu.make_async_copy(s, d, load_sem.at[i]) for i, (s, d) in enumerate(
        ((wd_hbm, wd), (h1_hbm, h1), (h3_hbm, h3), (wg_hbm, wg), (wu_hbm, wu)))]
    for cp in loads:
        cp.start()

    barrier = pltpu.get_barrier_semaphore()
    pl.semaphore_signal(barrier, inc=1, device_id=dev(z, y, oc), device_id_type=MESH)
    pl.semaphore_signal(barrier, inc=1, device_id=dev(z, oy, c), device_id_type=MESH)

    @pl.when(z > 0)
    def _():
        pl.semaphore_signal(barrier, inc=1, device_id=dev(z - 1, y, c), device_id_type=MESH)

    @pl.when(z < NZ - 1)
    def _():
        pl.semaphore_signal(barrier, inc=1, device_id=dev(z + 1, y, c), device_id_type=MESH)

    pl.semaphore_wait(barrier, 3 + z * (NZ - 1 - z) // 2)

    def ag_copies(src, msrc, hid, way, target):
        return (pltpu.make_async_remote_copy(src, gat.at[hid], ag_send.at[hid, way], ag_recv.at[hid],
                                             device_id=target, device_id_type=MESH),
                pltpu.make_async_remote_copy(msrc, met.at[hid], mt_send.at[hid, way], mt_recv.at[hid],
                                             device_id=target, device_id_type=MESH))

    def start(copies):
        for cp in copies:
            cp.start()

    def ag_wait(hid):
        for cp in ag_copies(gat.at[hid], met.at[hid], hid, 0, dev(z, y, oc)):
            cp.wait_recv()

    @pl.when(z < NZ - 1)
    def _():
        start(ag_copies(dy_ref, meta_ref, me, 2, dev(z + 1, y, c)))

    @pl.when(z > 0)
    def _():
        start(ag_copies(dy_ref, meta_ref, me, 3, dev(z - 1, y, c)))

    start(ag_copies(dy_ref, meta_ref, me, 1, dev(z, oy, c)))
    start(ag_copies(dy_ref, meta_ref, me, 0, dev(z, y, oc)))
    gat[me] = dy_ref[...]
    met[me] = meta_ref[...]

    def arrive(p, yy):
        hid = home(p, yy, c)
        ag_wait(hid)
        blk, mblk = gat.at[hid], met.at[hid]

        @pl.when((p <= z) & (z < NZ - 1))
        def _():
            start(ag_copies(blk, mblk, hid, 2, dev(z + 1, y, c)))

        @pl.when((p >= z) & (z > 0))
        def _():
            start(ag_copies(blk, mblk, hid, 3, dev(z - 1, y, c)))

        start(ag_copies(blk, mblk, hid, 0, dev(z, y, oc)))

    for cp in loads:
        cp.wait()

    def turn(e, carry):
        wd_t[e] = wd[e].T
        wg_t[e] = wg[e].T
        wu_t[e] = wu[e].T
        return carry

    lax.fori_loop(0, 2, turn, 0)

    def xs_copy(chip):
        return pltpu.make_async_remote_copy(xd.at[chip, oc], xr.at[chip], xs_sem.at[chip], xr_sem.at[chip],
                                            device_id=dev(z, y, oc), device_id_type=MESH)

    def out_copies(chip):
        rows = pl.ds(chip * 2 * cap, 2 * cap)
        return [pltpu.make_async_copy(s.at[:, rows], d.at[:, rows], out_sem.at[i, chip]) for i, (s, d) in enumerate(
            ((dyd, dyd_hbm), (act, act_hbm), (dh1, dh1_hbm), (dh3, dh3_hbm)))]

    slot = lax.broadcasted_iota(jnp.int32, (cap, 1), 0).astype(F32)

    def group(chip):
        first = (me * 2 * cap).astype(F32)
        rows = pl.ds(chip * 2 * cap, 2 * cap)
        picks, row_gate = [], []
        for e in range(2):
            for h in range(2):
                want = slot + (first + float(e * cap))
                hit = jnp.zeros((cap, tok), F32)
                gsum = jnp.zeros((cap, tok), F32)
                for j in range(top):
                    same = met[chip * 2 + h, j:j + 1, :] == want
                    hit = jnp.where(same, 1.0, hit)
                    gsum = jnp.where(same, met[chip * 2 + h, top + j:top + j + 1, :], gsum)
                row_gate.append(jnp.sum(gsum, axis=1, keepdims=True))
                none = jnp.zeros((cap, tok), F32)
                picks.append(jnp.concatenate([hit, none] if h == 0 else [none, hit], axis=1))
        pick = jnp.concatenate(picks, axis=0).astype(BF16)
        gate = jnp.concatenate(row_gate, axis=0)
        pair = jnp.concatenate([gat[chip * 2], gat[chip * 2 + 1]], axis=0)
        picked = dot(pick, pair)
        rows_dy = (picked * gate).astype(BF16)
        for e in range(2):
            dy_e = rows_dy[e * 2 * cap:(e + 1) * 2 * cap]
            dyd[e, rows] = dy_e
            d_act = dot(dy_e, wd_t[e]).astype(BF16).astype(F32)
            gate_f = h1[e, rows].astype(F32)
            up_f = h3[e, rows].astype(F32)
            sig = jax.nn.sigmoid(gate_f)
            silu = gate_f * sig
            act[e, rows] = (silu * up_f).astype(BF16)
            d1 = (d_act * up_f * sig * (1.0 + gate_f * (1.0 - sig))).astype(BF16)
            d3 = (d_act * silu).astype(BF16)
            dh1[e, rows] = d1
            dh3[e, rows] = d3
            d_x = (dot(d1, wg_t[e]) + dot(d3, wu_t[e])).astype(BF16)
            for h in range(2):
                xd[chip, h, e * cap:(e + 1) * cap] = d_x[h * cap:(h + 1) * cap]
        xs_copy(chip).start()
        for cp in out_copies(chip):
            cp.start()

    row_id = lax.broadcasted_iota(jnp.int32, (2 * cap, 1), 0).astype(F32)

    def partial(chip):
        hid = chip * 2 + c
        xs_copy(chip).wait_recv()
        want = jnp.concatenate([row_id + (me * 2 * cap).astype(F32),
                                row_id + ((me + 1 - 2 * c) * 2 * cap).astype(F32)], axis=0)
        hit = jnp.zeros((4 * cap, tok), F32)
        for j in range(top):
            hit = jnp.where(met[hid, j:j + 1, :] == want, 1.0, hit)
        vals = jnp.concatenate([xd[chip, c], xr[chip]], axis=0)
        return lax.dot_general(hit.astype(BF16), vals, (((0,), (0,)), ((), ())), preferred_element_type=F32)

    chunk = tok // NR

    def keep(side, k, chip):
        part = partial(chip)
        for i in range(NR):
            sp[side, k, i] = part[i * chunk:(i + 1) * chunk]

    def y_copy(k, i):
        return pltpu.make_async_remote_copy(sp.at[1, k, i], ry.at[k, i], sy_sem.at[k, i], ry_sem.at[k, i],
                                            device_id=dev(z, oy, c), device_id_type=MESH)

    def z_copy(k, i, target_z, to_slot):
        return pltpu.make_async_remote_copy(sp.at[0, k, i], rz.at[to_slot, i], sz_sem.at[k, i], rz_sem.at[to_slot, i],
                                            device_id=dev(target_z, y, c), device_id_type=MESH)

    def z_wait(from_slot, i):
        z_copy(0, i, z, from_slot).wait_recv()

    inner = z * (NZ - 1 - z) // 2
    at_end = inner == 0
    inside = inner == 1

    def pass_on(k, i):
        p = line_pos(z, k)
        way = jnp.where(p > z, 1, -1)
        behind = z - way
        ahead = z + way
        to_slot = jnp.where(ahead == p, jnp.where(way > 0, NZ, NZ + 1), p)
        y_copy(k, i).wait_recv()
        sp[0, k, i] += ry[k, i]

        @pl.when((behind >= 0) & (behind < NZ))
        def _():
            z_wait(p, i)
            sp[0, k, i] += rz[p, i]

        z_copy(k, i, ahead, to_slot).start()

    def step(n, carry):
        is3 = (n + 5) // 8 - (n + 4) // 8
        is4 = (n + 4) // 8 - (n + 3) // 8
        k = n // 2 + inner * (is3 - is4)
        side = n % 2 - inner * (is3 - is4)
        yy = y + side - 2 * y * side
        p = line_pos(z, k)

        @pl.when(n > 0)
        def _():
            arrive(p, yy)

        ag_wait(home(p, yy, oc))
        group(p * 2 + yy)

        @pl.when(side == 1)
        def _():
            keep(0, k, p * 2 + y)
            keep(1, k, p * 2 + oy)
            for i in range(NR // 2):
                y_copy(k, i).start()

            @pl.when(k > 0)
            def _():
                for i in range(NR // 2, NR):
                    y_copy(k, i).start()

            @pl.when(k == NZ - 1)
            def _():
                for i in range(NR // 2, NR):
                    y_copy(0, i).start()

        @pl.when((n == 4) & at_end)
        def _():
            pass_on(1, 0)

        @pl.when((n == 5) & at_end)
        def _():
            pass_on(1, 1)
            pass_on(1, 2)

        @pl.when((n == 6) & at_end)
        def _():
            pass_on(1, 3)
            pass_on(2, 0)
            pass_on(2, 1)

        return carry

    lax.fori_loop(0, 2 * NZ, step, 0)

    @pl.when(at_end)
    def _():
        pass_on(2, 2)
        pass_on(2, 3)
        for i in range(NR):
            pass_on(3, i)

    @pl.when(inside)
    def _():
        for i in range(NR):
            pass_on(2, i)
        for i in range(NR):
            pass_on(3, i)
            pass_on(1, i)

    for i in range(NR):
        y_copy(0, i).wait_recv()
        sp[0, 0, i] += ry[0, i]

        @pl.when(z > 0)
        def _():
            z_wait(NZ, i)
            sp[0, 0, i] += rz[NZ, i]

        @pl.when(z < NZ - 1)
        def _():
            z_wait(NZ + 1, i)
            sp[0, 0, i] += rz[NZ + 1, i]

        dx_ref[i * chunk:(i + 1) * chunk] = sp[0, 0, i].astype(BF16)

    def ag_sent(hid, way):
        for cp in ag_copies(gat.at[hid], met.at[hid], hid, way, dev(z, y, oc)):
            cp.wait_send()

    ag_sent(me, 1)
    for k in range(NZ):
        p = line_pos(z, k)
        for yy in range(2):
            hid = home(p, yy, c)
            ag_sent(hid, 0)

            @pl.when((p <= z) & (z < NZ - 1))
            def _():
                ag_sent(hid, 2)

            @pl.when((p >= z) & (z > 0))
            def _():
                ag_sent(hid, 3)

        for i in range(NR):
            y_copy(k, i).wait_send()
            if k:
                z_copy(k, i, z, 0).wait_send()

    def drain(chip, carry):
        xs_copy(chip).wait_send()
        for cp in out_copies(chip):
            cp.wait()
        return carry

    lax.fori_loop(0, 2 * NZ, drain, 0)


def exchange(dy, meta, h1, h3, wg, wu, wd, cap, top):
    tok, width = dy.shape
    n_exp, rows, ff = h1.shape
    homes = rows // cap
    chips = homes // 2
    chunk = tok // NR
    dma = pltpu.SemaphoreType.DMA
    any_spec = pl.BlockSpec(memory_space=pl.ANY)
    vmem_spec = pl.BlockSpec(memory_space=pltpu.VMEM)
    return pl.pallas_call(
        functools.partial(exchange_kernel, tok, cap, top),
        out_shape=(jax.ShapeDtypeStruct((tok, width), BF16),
                   jax.ShapeDtypeStruct((n_exp, rows, width), BF16),
                   jax.ShapeDtypeStruct((n_exp, rows, ff), BF16),
                   jax.ShapeDtypeStruct((n_exp, rows, ff), BF16),
                   jax.ShapeDtypeStruct((n_exp, rows, ff), BF16)),
        in_specs=[vmem_spec] * 2 + [any_spec] * 5,
        out_specs=(vmem_spec,) + (any_spec,) * 4,
        scratch_shapes=[
            pltpu.VMEM((homes, tok, width), BF16),
            pltpu.VMEM((homes, 2 * top, tok), F32),
            pltpu.VMEM(h1.shape, BF16),
            pltpu.VMEM(h3.shape, BF16),
            pltpu.VMEM(wg.shape, BF16),
            pltpu.VMEM(wu.shape, BF16),
            pltpu.VMEM(wd.shape, BF16),
            pltpu.VMEM((n_exp, ff, width), BF16),
            pltpu.VMEM((n_exp, ff, width), BF16),
            pltpu.VMEM((n_exp, width, ff), BF16),
            pltpu.VMEM((n_exp, rows, width), BF16),
            pltpu.VMEM((n_exp, rows, ff), BF16),
            pltpu.VMEM((n_exp, rows, ff), BF16),
            pltpu.VMEM((n_exp, rows, ff), BF16),
            pltpu.VMEM((chips, 2, n_exp * cap, width), BF16),
            pltpu.VMEM((chips, n_exp * cap, width), BF16),
            pltpu.VMEM((2, NZ, NR, chunk, width), F32),
            pltpu.VMEM((NZ, NR, chunk, width), F32),
            pltpu.VMEM((NZ + 2, NR, chunk, width), F32),
            dma((5,)), dma((4, chips)),
            dma((homes, 4)), dma((homes,)), dma((homes, 4)), dma((homes,)),
            dma((chips,)), dma((chips,)),
            dma((NZ, NR)), dma((NZ, NR)), dma((NZ, NR)), dma((NZ + 2, NR)),
        ],
        compiler_params=pltpu.CompilerParams(
            collective_id=0, has_side_effects=True, vmem_limit_bytes=62 * 2 ** 20),
    )(dy, meta, h1, h3, wg, wu, wd)


def weight_kernel(x_ref, dyd_ref, act_ref, dh1_ref, dh3_ref, gate_ref, up_ref, down_ref):
    def dot_0(a, b):
        return lax.dot_general(a, b, (((0,), (0,)), ((), ())), preferred_element_type=F32)

    gate_ref[0] = dot_0(x_ref[0], dh1_ref[0])
    up_ref[0] = dot_0(x_ref[0], dh3_ref[0])
    down_ref[0] = dot_0(act_ref[0], dyd_ref[0])


def weight_grads(x, dyd, act, dh1, dh3):
    n_exp, rows, width = x.shape
    ff = act.shape[2]
    tile = 256
    wide = pl.BlockSpec((1, rows, tile), lambda e, i: (e, 0, i))
    full = pl.BlockSpec((1, rows, ff), lambda e, i: (e, 0, 0))
    return pl.pallas_call(
        weight_kernel,
        grid=(n_exp, width // tile),
        in_specs=[wide, wide, full, full, full],
        out_specs=(pl.BlockSpec((1, tile, ff), lambda e, i: (e, i, 0)),
                   pl.BlockSpec((1, tile, ff), lambda e, i: (e, i, 0)),
                   pl.BlockSpec((1, ff, tile), lambda e, i: (e, 0, i))),
        out_shape=(jax.ShapeDtypeStruct((n_exp, width, ff), F32),
                   jax.ShapeDtypeStruct((n_exp, width, ff), F32),
                   jax.ShapeDtypeStruct((n_exp, ff, width), F32)),
        compiler_params=pltpu.CompilerParams(
            dimension_semantics=('arbitrary', 'arbitrary'), vmem_limit_bytes=60 * 2 ** 20),
    )(x, dyd, act, dh1, dh3)


def solution(mesh):
    ep_size = mesh.shape['ep']
    tok_spec = P(('dp', 'ep'), None)
    buf_spec = P(('dp', 'ep'), None, None)
    expert_spec = P('ep', None, None)

    def device_step(dy_loc, topk_idx, slot_idx, gates, y_back, x_disp, h1_disp, h3_disp, w_gate, w_up, w_down):
        cap = x_disp.shape[1] // ep_size
        top = topk_idx.shape[1]
        d_gates = jnp.einsum('td,tjd->tj', dy_loc, y_back, preferred_element_type=F32)
        flat = jnp.where(slot_idx >= 0, topk_idx * cap + slot_idx, -1).astype(F32)
        meta = jnp.concatenate([flat.T, gates.T], axis=0)
        dx_loc, dyd, act, dh1, dh3 = exchange(dy_loc, meta, h1_disp, h3_disp, w_gate, w_up, w_down, cap, top)
        dw_gate, dw_up, dw_down = weight_grads(x_disp, dyd, act, dh1, dh3)
        return dx_loc, d_gates, dw_gate, dw_up, dw_down

    return jax.shard_map(
        device_step, mesh=mesh,
        in_specs=(tok_spec, tok_spec, tok_spec, tok_spec, buf_spec, buf_spec, buf_spec, buf_spec,
                  expert_spec, expert_spec, expert_spec),
        out_specs=(tok_spec, tok_spec, buf_spec, buf_spec, buf_spec),
        check_vma=False)
```

```python
import functools

import jax
import jax.numpy as jnp
from jax import lax
from jax.experimental import pallas as pl
from jax.experimental.pallas import tpu as pltpu
from jax.sharding import PartitionSpec as P

MESH = pl.DeviceIdType.MESH
F32 = jnp.float32
BF16 = jnp.bfloat16
NZ = 4
NR = 4


def line_pos(z, k):
    edge = z * (3 - z) // 2
    far = z // 2
    is0 = (3 - k) // 3
    is1 = (k + 2) // 3 - (k + 1) // 3
    q = k + edge * is0 - edge * is1
    return q + 3 * far - 2 * far * q


def dot(a, b):
    return jnp.dot(a, b, preferred_element_type=F32)


def exchange_kernel(tok, cap, top,
                    dy_ref, topk_ref, slot_ref, gates_ref, yb_hbm, x_hbm, h1_hbm, h3_hbm, wg_hbm, wu_hbm, wd_hbm,
                    dx_ref, dgate_ref, dwg_ref, dwu_ref, dwd_ref,
                    gat, met, mine, h1, h3, wg_t, wu_t, wd_t, xb, yb, dyd, act, xd, xr, sp, ry, rz, lanes,
                    load_sem, ag_send, ag_recv, mt_send, mt_recv,
                    xs_sem, xr_sem, sy_sem, ry_sem, sz_sem, rz_sem):
    me = lax.axis_index('ep')
    dp = lax.axis_index('dp')
    z, y, c = me // 4, (me // 2) % 2, me % 2
    oy, oc = 1 - y, 1 - c

    def dev(z_, y_, c_):
        return (dp, (z_ * 2 + y_) * 2 + c_)

    def home(z_, y_, c_):
        return (z_ * 2 + y_) * 2 + c_

    ff = h1.shape[2]
    raw_d, raw_g, raw_u = dyd.at[:, 0:ff, :], xb.at[:, :, 0:ff], xb.at[:, :, ff:2 * ff]
    loads = [pltpu.make_async_copy(s, d, load_sem.at[i]) for i, (s, d) in enumerate(
        ((wd_hbm, raw_d), (wg_hbm, raw_g), (wu_hbm, raw_u), (h1_hbm, h1), (h3_hbm, h3), (yb_hbm, yb)))]
    for cp in loads:
        cp.start()
    x_load = pltpu.make_async_copy(x_hbm, xb, load_sem.at[6])

    mine[0:top] = jnp.where(slot_ref[...] >= 0, topk_ref[...] * cap + slot_ref[...], -1).astype(F32)
    mine[top:2 * top] = gates_ref[...]

    barrier = pltpu.get_barrier_semaphore()
    pl.semaphore_signal(barrier, inc=1, device_id=dev(z, y, oc), device_id_type=MESH)
    pl.semaphore_signal(barrier, inc=1, device_id=dev(z, oy, c), device_id_type=MESH)

    @pl.when(z > 0)
    def _():
        pl.semaphore_signal(barrier, inc=1, device_id=dev(z - 1, y, c), device_id_type=MESH)

    @pl.when(z < NZ - 1)
    def _():
        pl.semaphore_signal(barrier, inc=1, device_id=dev(z + 1, y, c), device_id_type=MESH)

    @pl.when((z == 0) | (z == NZ - 1))
    def _():
        pl.semaphore_signal(barrier, inc=1, device_id=dev(NZ - 1 - z, y, c), device_id_type=MESH)

    pl.semaphore_wait(barrier, 4)

    def ag_copies(src, msrc, hid, way, target):
        return (pltpu.make_async_remote_copy(src, gat.at[hid], ag_send.at[hid, way], ag_recv.at[hid],
                                             device_id=target, device_id_type=MESH),
                pltpu.make_async_remote_copy(msrc, met.at[hid], mt_send.at[hid, way], mt_recv.at[hid],
                                             device_id=target, device_id_type=MESH))

    def start(copies):
        for cp in copies:
            cp.start()

    def ag_wait(hid):
        for cp in ag_copies(gat.at[hid], met.at[hid], hid, 0, dev(z, y, oc)):
            cp.wait_recv()

    @pl.when(z < NZ - 1)
    def _():
        start(ag_copies(dy_ref, mine, me, 2, dev(z + 1, y, c)))

    @pl.when(z > 0)
    def _():
        start(ag_copies(dy_ref, mine, me, 3, dev(z - 1, y, c)))

    start(ag_copies(dy_ref, mine, me, 1, dev(z, oy, c)))
    start(ag_copies(dy_ref, mine, me, 0, dev(z, y, oc)))
    gat[me] = dy_ref[...]
    met[me] = mine[...]

    def arrive(p, yy):
        hid = home(p, yy, c)
        ag_wait(hid)
        blk, mblk = gat.at[hid], met.at[hid]

        @pl.when((p <= z) & (z < NZ - 1))
        def _():
            start(ag_copies(blk, mblk, hid, 2, dev(z + 1, y, c)))

        @pl.when((p >= z) & (z > 0))
        def _():
            start(ag_copies(blk, mblk, hid, 3, dev(z - 1, y, c)))

        start(ag_copies(blk, mblk, hid, 0, dev(z, y, oc)))

    def turn(e, carry):
        wd_t[e] = dyd[e, 0:ff, :].T
        wg_t[e] = xb[e, :, 0:ff].T
        wu_t[e] = xb[e, :, ff:2 * ff].T
        return carry

    with jax.named_scope('turn'):
        for cp in loads:
            cp.wait()
        lax.fori_loop(0, 2, turn, 0)
        x_load.start()

    def xs_copy(chip):
        return pltpu.make_async_remote_copy(xd.at[chip, oc], xr.at[chip], xs_sem.at[chip], xr_sem.at[chip],
                                            device_id=dev(z, y, oc), device_id_type=MESH)

    slot = lax.broadcasted_iota(jnp.int32, (cap, 1), 0).astype(F32)

    def group(chip):
        first = (me * 2 * cap).astype(F32)
        rows = pl.ds(chip * 2 * cap, 2 * cap)
        picks, row_gate = [], []
        for e in range(2):
            for h in range(2):
                want = slot + (first + float(e * cap))
                hit = jnp.zeros((cap, tok), F32)
                gsum = jnp.zeros((cap, tok), F32)
                for j in range(top):
                    same = met[chip * 2 + h, j:j + 1, :] == want
                    hit = jnp.where(same, 1.0, hit)
                    gsum = jnp.where(same, met[chip * 2 + h, top + j:top + j + 1, :], gsum)
                row_gate.append(jnp.sum(gsum, axis=1, keepdims=True))
                none = jnp.zeros((cap, tok), F32)
                picks.append(jnp.concatenate([hit, none] if h == 0 else [none, hit], axis=1))
        pick = jnp.concatenate(picks, axis=0).astype(BF16)
        gate = jnp.concatenate(row_gate, axis=0)
        pair = jnp.concatenate([gat[chip * 2], gat[chip * 2 + 1]], axis=0)
        picked = dot(pick, pair)
        rows_dy = (picked * gate).astype(BF16)
        for e in range(2):
            dy_e = rows_dy[e * 2 * cap:(e + 1) * 2 * cap]
            dyd[e, rows] = dy_e
            d_act = dot(dy_e, wd_t[e]).astype(BF16).astype(F32)
            gate_f = h1[e, rows].astype(F32)
            up_f = h3[e, rows].astype(F32)
            sig = jax.nn.sigmoid(gate_f)
            silu = gate_f * sig
            act[e, rows] = (silu * up_f).astype(BF16)
            d1 = (d_act * up_f * sig * (1.0 + gate_f * (1.0 - sig))).astype(BF16)
            d3 = (d_act * silu).astype(BF16)
            h1[e, rows] = d1
            h3[e, rows] = d3
            d_x = (dot(d1, wg_t[e]) + dot(d3, wu_t[e])).astype(BF16)
            for h in range(2):
                xd[chip, h, e * cap:(e + 1) * cap] = d_x[h * cap:(h + 1) * cap]
        xs_copy(chip).start()

    row_id = lax.broadcasted_iota(jnp.int32, (2 * cap, 1), 0).astype(F32)

    def partial(chip):
        hid = chip * 2 + c
        xs_copy(chip).wait_recv()
        want = jnp.concatenate([row_id + (me * 2 * cap).astype(F32),
                                row_id + ((me + 1 - 2 * c) * 2 * cap).astype(F32)], axis=0)
        hit = jnp.zeros((4 * cap, tok), F32)
        for j in range(top):
            hit = jnp.where(met[hid, j:j + 1, :] == want, 1.0, hit)
        vals = jnp.concatenate([xd[chip, c], xr[chip]], axis=0)
        return lax.dot_general(hit.astype(BF16), vals, (((0,), (0,)), ((), ())), preferred_element_type=F32)

    chunk = tok // NR

    def keep(side, k, chip):
        part = partial(chip)
        for i in range(NR):
            sp[side, k, i] = part[i * chunk:(i + 1) * chunk]

    def y_copy(k, i):
        return pltpu.make_async_remote_copy(sp.at[1, k, i], ry.at[k, i], sy_sem.at[k, i], ry_sem.at[k, i],
                                            device_id=dev(z, oy, c), device_id_type=MESH)

    def z_copy(k, i, target_z, to_slot):
        return pltpu.make_async_remote_copy(sp.at[0, k, i], rz.at[to_slot, i], sz_sem.at[k, i], rz_sem.at[to_slot, i],
                                            device_id=dev(target_z, y, c), device_id_type=MESH)

    def z_wait(from_slot, i):
        z_copy(0, i, z, from_slot).wait_recv()

    inner = z * (NZ - 1 - z) // 2
    at_end = inner == 0
    inside = inner == 1

    def pass_on(k, i):
        p = line_pos(z, k)
        way = jnp.where(p > z, 1, -1)
        behind = z - way
        ahead = z + way
        across = at_end & (k == NZ - 1)
        to_slot = jnp.where(ahead == p, jnp.where(way > 0, NZ, NZ + 1), p)
        y_copy(k, i).wait_recv()
        sp[0, k, i] += ry[k, i]

        @pl.when((behind >= 0) & (behind < NZ) & (k < NZ - 1))
        def _():
            z_wait(p, i)
            sp[0, k, i] += rz[p, i]

        z_copy(k, i, jnp.where(across, p, ahead), jnp.where(across, NZ + 2, to_slot)).start()

    tile = 256
    per = (2 * ff) // tile

    def dot_0(a_, b_):
        return lax.dot_general(a_, b_, (((0,), (0,)), ((), ())), preferred_element_type=F32)

    def weight_unit(u):
        @pl.when(u < 2 * per)
        def _():
            e, m = u // per, u % per
            cols = pl.ds(pl.multiple_of(m * tile, tile), tile)
            part = xb[e, :, cols]
            dwg_ref[e, cols] = dot_0(part, h1[e])
            dwu_ref[e, cols] = dot_0(part, h3[e])

        @pl.when(u >= 2 * per)
        def _():
            v = u - 2 * per
            e, m = v // (per // 2), v % (per // 2)
            cols = pl.ds(pl.multiple_of(m * tile, tile), tile)
            dwd_ref[e, cols] = dot_0(act[e, :, cols], dyd[e])

    n_unit = 3 * per

    def gate_rows(i, carry):
        few = 8
        t0 = pl.multiple_of(i * few, few)
        d = dy_ref[pl.ds(t0, few)].astype(F32)
        prod = yb[pl.ds(t0, few)].astype(F32) * d[:, None, :]
        acc = prod[:, :, 0:128]
        for q in range(1, prod.shape[2] // 128):
            acc = acc + prod[:, :, q * 128:(q + 1) * 128]
        lanes[pl.ds(pl.multiple_of(t0 * top, few * top), few * top)] = acc.reshape(few * top, 128)
        return carry

    def gate_grads():
        lax.fori_loop(0, tok // 8, gate_rows, 0)
        for j in range(top):
            dgate_ref[j:j + 1] = jnp.sum(lanes[pl.ds(j, tok, stride=top)].T, axis=0, keepdims=True)

    def place(n, mid):
        is3 = (n + 5) // 8 - (n + 4) // 8
        is4 = (n + 4) // 8 - (n + 3) // 8
        k = n // 2 + mid * (is3 - is4)
        side = n % 2 - mid * (is3 - is4)
        return k, side

    def arrive_at(n, mid):
        k, side = place(n, mid)
        with jax.named_scope('arrive'):
            arrive(line_pos(z, k), y + side - 2 * y * side)

    def y_send(k, lo, hi):
        for i in range(lo, hi):
            y_copy(k, i).start()

    mid_arrivals = {1: (1, 2, 3), 4: (4, 5), 6: (6,), 7: (7,)}
    mid_keeps = {2: 0, 5: 1, 6: 2, 7: 3}
    half = NR // 2

    def step(n, carry):
        k, side = place(n, inner)
        p = line_pos(z, k)
        yy = y + side - 2 * y * side

        @pl.when(at_end & (n > 0))
        def _():
            arrive_at(n, 0)

        for n0, blocks in mid_arrivals.items():
            @pl.when(inside & (n == n0))
            def _():
                for m in blocks:
                    arrive_at(m, 1)

        @pl.when(at_end & (n == 7))
        def _():
            for i in range(half):
                pass_on(2, i)

        with jax.named_scope('other_core'):
            ag_wait(home(p, yy, oc))
        with jax.named_scope('group'):
            group(p * 2 + yy)

        mid_keep = (n == 2) | (n == 5) | (n == 6) | (n == 7)

        @pl.when((at_end & (side == 1)) | (inside & mid_keep))
        def _():
            kk = jnp.where(at_end, k, (n - 1) // 4 + n // 6 + n // 7)
            q = line_pos(z, kk)
            with jax.named_scope('keep'):
                keep(1, kk, q * 2 + oy)

                @pl.when(kk == 0)
                def _():
                    y_send(0, 0, half)

                @pl.when((kk == 1) | (kk == 3) | (at_end & (kk == 2)))
                def _():
                    y_send(kk, 0, NR)

                @pl.when(inside & (kk == 3))
                def _():
                    y_send(2, 0, NR)

                @pl.when(kk == 3)
                def _():
                    y_send(0, half, NR)

                keep(0, kk, q * 2 + y)

        @pl.when((n == 4) & at_end)
        def _():
            pass_on(1, 0)

        @pl.when((n == 5) & at_end)
        def _():
            for i in range(1, NR):
                pass_on(1, i)

        return carry

    lax.fori_loop(0, 2 * NZ, step, 0)

    x_load.wait()
    end_order = [(2, i) for i in range(half, NR)] + [(3, i) for i in range(NR)]
    mid_order = [(3, 0), (3, 1), (1, 0), (3, 2), (1, 1), (3, 3), (1, 2), (2, 0), (1, 3), (2, 1), (2, 2), (2, 3)]

    def late(m, carry):
        with jax.named_scope('weights'):
            weight_unit(m)

        with jax.named_scope('pass_on'):
            for m0, (k, i) in enumerate(end_order):
                @pl.when(at_end & (m == m0))
                def _():
                    pass_on(k, i)

            for m0, (k, i) in enumerate(mid_order):
                @pl.when(inside & (m == m0))
                def _():
                    pass_on(k, i)

        return carry

    lax.fori_loop(0, n_unit, late, 0)
    with jax.named_scope('gates'):
        gate_grads()

    for i in range(NR):
        with jax.named_scope('final'):
            y_copy(0, i).wait_recv()
        sp[0, 0, i] += ry[0, i]

        @pl.when(z > 0)
        def _():
            z_wait(NZ, i)
            sp[0, 0, i] += rz[NZ, i]

        @pl.when(z < NZ - 1)
        def _():
            z_wait(NZ + 1, i)
            sp[0, 0, i] += rz[NZ + 1, i]

        @pl.when(at_end)
        def _():
            z_wait(NZ + 2, i)
            sp[0, 0, i] += rz[NZ + 2, i]

        dx_ref[i * chunk:(i + 1) * chunk] = sp[0, 0, i].astype(BF16)

    def ag_sent(hid, way):
        for cp in ag_copies(gat.at[hid], met.at[hid], hid, way, dev(z, y, oc)):
            cp.wait_send()

    ag_sent(me, 1)
    for k in range(NZ):
        p = line_pos(z, k)
        for yy in range(2):
            hid = home(p, yy, c)
            ag_sent(hid, 0)

            @pl.when((p <= z) & (z < NZ - 1))
            def _():
                ag_sent(hid, 2)

            @pl.when((p >= z) & (z > 0))
            def _():
                ag_sent(hid, 3)

        for i in range(NR):
            y_copy(k, i).wait_send()
            if k:
                z_copy(k, i, z, 0).wait_send()

    def drain(chip, carry):
        xs_copy(chip).wait_send()
        return carry

    lax.fori_loop(0, 2 * NZ, drain, 0)


def exchange(dy, topk, slot, gates, yb, x, h1, h3, wg, wu, wd, cap):
    tok, width = dy.shape
    top = topk.shape[0]
    n_exp, rows, ff = h1.shape
    homes = rows // cap
    chips = homes // 2
    chunk = tok // NR
    dma = pltpu.SemaphoreType.DMA
    any_spec = pl.BlockSpec(memory_space=pl.ANY)
    vmem_spec = pl.BlockSpec(memory_space=pltpu.VMEM)
    return pl.pallas_call(
        functools.partial(exchange_kernel, tok, cap, top),
        out_shape=(pltpu.VMEM((tok, width), BF16),
                   pltpu.VMEM((top, tok), F32),
                   pltpu.VMEM((n_exp, width, ff), F32),
                   pltpu.VMEM((n_exp, width, ff), F32),
                   pltpu.VMEM((n_exp, ff, width), F32)),
        in_specs=[vmem_spec] * 4 + [any_spec] * 7,
        out_specs=(vmem_spec,) * 5,
        scratch_shapes=[
            pltpu.VMEM((homes, tok, width), BF16),
            pltpu.VMEM((homes, 2 * top, tok), F32),
            pltpu.VMEM((2 * top, tok), F32),
            pltpu.VMEM(h1.shape, BF16),
            pltpu.VMEM(h3.shape, BF16),
            pltpu.VMEM((n_exp, ff, width), BF16),
            pltpu.VMEM((n_exp, ff, width), BF16),
            pltpu.VMEM((n_exp, width, ff), BF16),
            pltpu.VMEM(x.shape, BF16),
            pltpu.VMEM(yb.shape, BF16),
            pltpu.VMEM((n_exp, rows, width), BF16),
            pltpu.VMEM((n_exp, rows, ff), BF16),
            pltpu.VMEM((chips, 2, n_exp * cap, width), BF16),
            pltpu.VMEM((chips, n_exp * cap, width), BF16),
            pltpu.VMEM((2, NZ, NR, chunk, width), F32),
            pltpu.VMEM((NZ, NR, chunk, width), F32),
            pltpu.VMEM((NZ + 3, NR, chunk, width), F32),
            pltpu.VMEM((tok * top, 128), F32),
            dma((7,)),
            dma((homes, 4)), dma((homes,)), dma((homes, 4)), dma((homes,)),
            dma((chips,)), dma((chips,)),
            dma((NZ, NR)), dma((NZ, NR)), dma((NZ, NR)), dma((NZ + 3, NR)),
        ],
        compiler_params=pltpu.CompilerParams(
            collective_id=0, has_side_effects=True, vmem_limit_bytes=48 * 2 ** 20),
    )(dy, topk, slot, gates, yb, x, h1, h3, wg, wu, wd)


def solution(mesh):
    ep_size = mesh.shape['ep']
    tok_spec = P(('dp', 'ep'), None)
    buf_spec = P(('dp', 'ep'), None, None)
    expert_spec = P('ep', None, None)

    def device_step(dy_loc, topk_idx, slot_idx, gates, y_back, x_disp, h1_disp, h3_disp, w_gate, w_up, w_down):
        cap = x_disp.shape[1] // ep_size
        dx_loc, d_gates, dw_gate, dw_up, dw_down = exchange(
            dy_loc, topk_idx.T, slot_idx.T, gates.T, y_back, x_disp, h1_disp, h3_disp,
            w_gate, w_up, w_down, cap)
        return dx_loc, d_gates.T, dw_gate, dw_up, dw_down

    return jax.shard_map(
        device_step, mesh=mesh,
        in_specs=(tok_spec, tok_spec, tok_spec, tok_spec, buf_spec, buf_spec, buf_spec, buf_spec,
                  expert_spec, expert_spec, expert_spec),
        out_specs=(tok_spec, tok_spec, buf_spec, buf_spec, buf_spec),
        check_vma=False)
```
